32 devices in a mesh: grp: 4 (over x, core), sub: 8 (over z, y).
Axes of the slice: x: 2, y: 2, z: 4, core: 2. Of those that a mesh axis runs over, the one named last changes fastest.
Arguments:
- snapshots: bfloat16 [2048, 2, 32, 128], P(None, None, ('grp', 'sub')), may hold values from -6 to 6
- steering: bfloat16 [32, 2, 128, 64], P(('grp', 'sub')), may hold values from -0.375 to 0.375
- combining: bfloat16 [32, 2, 64, 1024], P(('grp', 'sub')), may hold values from -0.09375 to 0.09375
- beam_list: int32 [1024], replicated, may hold values from 0 to 1023, each once
Outputs:
- beams_out: bfloat16 [2, 2048, 1024], P(None, ('grp', 'sub'))
The draws below stay inside these ranges and needn't reach their ends.
Inputs may be any that keep to these rules, and one draw needn't show every extreme that they name: `beam_list`: each of the 1024 beams appears once.
All inputs are finite; a program needn't handle non-finite values.
Results may differ from the reference program's by a relative error of at most 0.0065.
Values may be sent and summed in bfloat16 or wider, within the bound.
No kernel may reach another device: no remote copies, remote signals or barrier semaphores. Data moves between devices by JAX's collectives and lax.ppermute only.
A program may use at most 128 MiB of HBM per device.

```python
import jax
import jax.numpy as jnp
from jax import lax

EL = 128
PB = 64
NBEAM = 1024
SNAP = 2048
SUBS = 32


def level_of(stream_key, extent, pieces, smallest, largest):
    def one(dim, blocks):
        draws = jax.random.uniform(jax.random.fold_in(jax.random.fold_in(stream_key, 6), dim), (blocks,), jnp.float32, smallest / len(pieces), largest / len(pieces))
        return jnp.repeat(jnp.exp(draws), extent[dim] // blocks).reshape((-1,) + (1,) * (len(extent) - dim - 1))

    factor_of = one(*pieces[0])
    for cut in pieces[1:]:
        factor_of = factor_of * one(*cut)
    return factor_of


def noise(rng, dims, width, limit, shards=(), kind=jnp.bfloat16):
    result = jax.random.normal(rng, dims, jnp.float32) * width
    if len(shards) > 0:
        result = level_of(rng, dims, shards, -0.22, 0.18) * result
    return jnp.clip(result, min=-limit, max=limit).astype(kind)


def setup_inputs(seed: int = 0) -> dict:
    keys = jax.random.split(jax.random.key(seed), 5)
    return {
        "snapshots": noise(keys[0], (SNAP, 2, SUBS, EL), 1.0, 6.0, ((2, 32),)),
        "steering": noise(keys[1], (SUBS, 2, EL, PB), (2 * EL) ** -0.5, 0.375, ((0, 32),)),
        "combining": noise(keys[2], (SUBS, 2, PB, NBEAM), (2 * SUBS * PB) ** -0.5, 0.09375, ((0, 32),)),
        "beam_list": jax.random.permutation(keys[3], NBEAM).astype(jnp.int32),
    }


def reference(snapshots, steering, combining, beam_list):
    ordered = jnp.take(combining, beam_list, axis=3)

    def accumulate(subarray, running):
        signal = lax.dynamic_index_in_dim(snapshots, subarray, 2, keepdims=False).astype(jnp.float32)
        steer_s = lax.dynamic_index_in_dim(steering, subarray, 0, keepdims=False).astype(jnp.float32)
        comb_s = lax.dynamic_index_in_dim(ordered, subarray, 0, keepdims=False).astype(jnp.float32)
        sig_real = signal[:, 0]
        sig_imag = signal[:, 1]
        beam_real = jnp.dot(sig_real, steer_s[0]) - jnp.dot(sig_imag, steer_s[1])
        beam_imag = jnp.dot(sig_real, steer_s[1]) + jnp.dot(sig_imag, steer_s[0])
        beam_real = lax.optimization_barrier(beam_real.astype(jnp.bfloat16)).astype(jnp.float32)
        beam_imag = lax.optimization_barrier(beam_imag.astype(jnp.bfloat16)).astype(jnp.float32)
        final_real = jnp.dot(beam_real, comb_s[0]) - jnp.dot(beam_imag, comb_s[1])
        final_imag = jnp.dot(beam_real, comb_s[1]) + jnp.dot(beam_imag, comb_s[0])
        return running + jnp.stack([final_real, final_imag])

    running = lax.fori_loop(0, SUBS, accumulate, jnp.zeros((2, SNAP, NBEAM), jnp.float32))
    return running.astype(jnp.bfloat16)
```

```python
import functools

import jax
import jax.numpy as jnp
from jax import lax
from jax.experimental import pallas as pl
from jax.experimental.pallas import tpu as pltpu
from jax.sharding import PartitionSpec as P

CHUNKS = 2
VMEM = pl.BlockSpec(memory_space=pltpu.VMEM)
F32 = jnp.float32
BF16 = jnp.bfloat16


class Place:
    def __init__(self, groups, subs):
        self.cores = 2
        self.xs = groups // 2
        self.ys = 2
        self.zs = subs // 2
        self.subs = subs
        self.plane = self.xs * self.ys

    def index(self, x, core, z, y):
        return ((x * self.cores + core) * self.zs + z) * self.ys + y

    def pairs(self, move):
        return [
            (self.index(x, core, z, y), self.index(*move(x, core, z, y)))
            for x in range(self.xs)
            for core in range(self.cores)
            for z in range(self.zs)
            for y in range(self.ys)
        ]

    def here(self):
        group = lax.axis_index("grp")
        sub = lax.axis_index("sub")
        return group // 2, lax.rem(group, 2), sub // 2, lax.rem(sub, 2)


def send(value, place, move):
    return lax.ppermute(value, ("grp", "sub"), place.pairs(move))


def plane_step(place, k):
    dx, dy = k // place.ys, k % place.ys
    return lambda x, core, z, y: ((x + dx) % place.xs, core, z, (y + dy) % place.ys)


def depth_step(place, k):
    return lambda x, core, z, y: (x, core, (z + k) % place.zs, y)


def core_step(x, core, z, y):
    return (x, 1 - core, z, y)


def dot(a, b, dims=((1,), (0,))):
    return lax.dot_general(a, b, (dims, ((), ())), preferred_element_type=F32)


def first_section(place, rows, snap_ref, steer_ref, *refs):
    out_refs, (low, high) = refs[:-2], refs[-2:]
    x, _, _, y = place.here()
    half = steer_ref.shape[0] // 2
    real, imag = steer_ref[:half], steer_ref[half:]
    weights = jnp.concatenate([real, imag, -imag, real], axis=0)
    width = 2 * half
    for k, out_ref in enumerate(out_refs):
        to_x = lax.rem(x + k // place.ys, place.xs)
        to_y = lax.rem(y + k % place.ys, place.ys)
        blocks = []
        for core in range(place.cores):
            for z in range(place.zs):
                start = place.index(to_x, core, z, to_y) * (2 * rows)
                blocks.append(snap_ref[pl.ds(pl.multiple_of(start, 2 * rows), 2 * rows), :])
        signal = jnp.concatenate(blocks, axis=0)
        count = signal.shape[0] // 2
        product = dot(signal, weights, ((1,), (1,)))
        low[...] = product[:, :width]
        high[...] = product[:, width:]
        even = low[pl.ds(0, count, 2), :]
        odd = high[pl.ds(1, count, 2), :]
        out_ref[...] = (even + odd).astype(BF16)


def order_beams(list_ref, comb_ref, *out_refs):
    beams = comb_ref.shape[1]
    step = beams // len(out_refs)
    weights = comb_ref[...]
    for c, out_ref in enumerate(out_refs):
        wanted = list_ref[:, c * step : (c + 1) * step]
        rows = lax.broadcasted_iota(jnp.int32, (beams, step), 0)
        pick = jnp.where(rows == wanted, 1.0, 0.0).astype(BF16)
        out_ref[...] = dot(weights, pick).astype(BF16)


def load_weights(comb_refs):
    parts = []
    for ref in comb_refs:
        half = ref.shape[0] // 2
        real, imag = ref[:half], ref[half:]
        parts.append(
            jnp.concatenate(
                [jnp.concatenate([real, imag], axis=1), jnp.concatenate([-imag, real], axis=1)],
                axis=0,
            )
        )
    return jnp.concatenate(parts, axis=0)


def other_core_share(place, *refs):
    count = place.plane
    part_refs, comb_refs, out_ref = refs[:count], refs[count : 2 * count], refs[2 * count]
    _, core, _, _ = place.here()
    rows = part_refs[0].shape[0] // place.cores
    start = pl.multiple_of((1 - core) * rows, rows)
    left = jnp.concatenate([ref[pl.ds(start, rows), :] for ref in part_refs], axis=1)
    out_ref[...] = dot(left, load_weights(comb_refs)).astype(BF16)


def own_core_share(place, *refs):
    count = place.plane
    part_refs, comb_refs = refs[:count], refs[count : 2 * count]
    got_ref = refs[2 * count]
    out_refs, scratch = refs[2 * count + 1 : -1], refs[-1]
    _, core, z, _ = place.here()
    rows = part_refs[0].shape[0] // place.cores
    start = pl.multiple_of(core * rows, rows)
    left = jnp.concatenate([ref[pl.ds(start, rows), :] for ref in part_refs], axis=1)
    scratch[...] = dot(left, load_weights(comb_refs)) + got_ref[...].astype(F32)
    block = rows // place.zs
    for k, out_ref in enumerate(out_refs):
        to_z = lax.rem(z + k, place.zs)
        piece = scratch[pl.ds(pl.multiple_of(to_z * block, block), block), :]
        out_ref[...] = piece.astype(out_ref.dtype)


def finish(depth, *refs):
    out_ref = refs[-1]
    chunks = len(refs[:-1]) // depth
    for c in range(chunks):
        terms = refs[c * depth : (c + 1) * depth]
        total = terms[0][...]
        for term in terms[1:]:
            total = total + term[...].astype(F32)
        total = total.astype(BF16)
        step = total.shape[1] // 2
        out_ref[0, :, c * step : (c + 1) * step] = total[:, :step]
        out_ref[1, :, c * step : (c + 1) * step] = total[:, step:]


def call(body, shapes, args, scratch=(), flops=0):
    moved = sum(a.size * a.dtype.itemsize for a in args)
    return pl.pallas_call(
        body,
        out_shape=shapes,
        in_specs=[VMEM] * len(args),
        out_specs=jax.tree.map(lambda _: VMEM, shapes),
        scratch_shapes=list(scratch),
        compiler_params=pltpu.CompilerParams(vmem_limit_bytes=16 * 2**20),
        cost_estimate=pl.CostEstimate(flops=flops, bytes_accessed=moved, transcendentals=0),
    )(*args)


def shards(snapshots, steering, combining, beam_list):
    place = Place(lax.axis_size("grp"), lax.axis_size("sub"))
    snaps, _, _, elements = snapshots.shape
    partials = steering.shape[3]
    beams = combining.shape[3]
    rows = snaps // (lax.axis_size("grp") * lax.axis_size("sub"))
    taken = rows * place.cores * place.zs
    shape = jax.ShapeDtypeStruct

    signal = snapshots.reshape(snaps * 2, elements)
    steer = jnp.transpose(steering[0], (0, 2, 1)).reshape(2 * partials, elements)
    comb = combining.reshape(2 * partials, beams)

    parts = call(
        functools.partial(first_section, place, rows),
        [shape((taken, 2 * partials), BF16)] * place.plane,
        (signal, steer),
        [pltpu.VMEM((2 * taken, 2 * partials), F32)] * 2,
        flops=2 * 2 * snaps * elements * 4 * partials,
    )
    parts = [parts[0]] + [
        send(parts[k], place, plane_step(place, k)) for k in range(1, place.plane)
    ]

    step = beams // CHUNKS
    ordered = call(
        order_beams,
        [shape((2 * partials, step), BF16)] * CHUNKS,
        (beam_list.reshape(1, beams), comb),
        flops=2 * 2 * partials * beams * beams,
    )

    terms = []
    for c in range(CHUNKS):
        combs = [ordered[c]] + [
            send(ordered[c], place, plane_step(place, k)) for k in range(1, place.plane)
        ]
        flops = 2 * taken // 2 * 2 * partials * place.plane * 2 * step
        mine = taken // place.cores
        share = call(
            functools.partial(other_core_share, place),
            shape((mine, 2 * step), BF16),
            (*parts, *combs),
            flops=flops,
        )
        got = send(share, place, core_step)
        pieces = call(
            functools.partial(own_core_share, place),
            [shape((rows, 2 * step), F32)] + [shape((rows, 2 * step), BF16)] * (place.zs - 1),
            (*parts, *combs, got),
            [pltpu.VMEM((mine, 2 * step), F32)],
            flops=flops,
        )
        terms.append(pieces[0])
        terms.extend(send(pieces[k], place, depth_step(place, k)) for k in range(1, place.zs))

    return call(
        functools.partial(finish, place.zs),
        shape((2, rows, beams), BF16),
        tuple(terms),
        flops=len(terms) * rows * 2 * step,
    )


def solution(mesh):
    placed = (
        P(None, None, ("grp", "sub"), None),
        P(("grp", "sub"), None, None, None),
        P(("grp", "sub"), None, None, None),
        P(),
    )
    return jax.shard_map(
        shards, mesh=mesh, in_specs=placed, out_specs=P(None, ("grp", "sub"), None), check_vma=False
    )
```
